512 devices in a mesh: ma: 64 (over z_lo, x, core), af: 8 (over y, z_hi).
Axes of the slice: x: 4, y: 4, z: 16 (z_hi: 2, z_lo: 8; z = z_hi * 8 + z_lo), core: 2. Of those that a mesh axis runs over, the one named last changes fastest.
Arguments:
- coeffs: bfloat16 [512, 512, 2049], P('ma', 'af'), parts along dimension 1, may hold values from -6 to 6
- legendre: bfloat16 [512, 256, 2049], P('ma'), may hold values from -0.1875 to 0.1875
- assign: int32 [512], P('ma'), may hold values from 0 to 511, each once
Outputs:
- fourier: float32 [512, 512, 1024], P('ma', 'af'), parts along dimension 1
The draws below stay inside these ranges and needn't reach their ends.
There are 8 independent parts, one for each index of `af`. The reference program is written for one: setup_inputs(seed, part) draws one part's arguments, and reference() takes and returns one part's arrays. A program takes and returns all parts, laid end to end along the dimension named above; an argument that names none is the same for every part. Nothing has to cross between parts.
Inputs may be any that keep to these rules, and one draw needn't show every extreme that they name: Slot s carries the wavenumbers assign[s] and 2047 - assign[s]; every pair appears once.
All inputs are finite; a program needn't handle non-finite values.
Results may differ from the reference program's by a relative error of at most 0.0003.
Values sent between devices are 32-bit elements; how exact they have to be, the bound alone decides.
A program may use at most 64 MiB of HBM per device.

```python
import jax
import jax.numpy as jnp
from jax import lax

TRUNC = 2047
PAIRS = 512
HLAT = 256
FIELDS = 32
KP = 2049
COLS = 64


def block_scale(key, extent, pieces, low, high):
    level, own = 1.0, jax.random.fold_in(key, 6)
    for dim, blocks in pieces:
        heights = jnp.exp(jax.random.uniform(jax.random.fold_in(own, dim), (blocks,), jnp.float32, low / len(pieces), high / len(pieces)))
        level = level * jnp.repeat(heights, extent[dim] // blocks).reshape([-1 if axis == dim else 1 for axis in range(len(extent))])
    return level


def centred(rng, shape, scale, most, shards=(), held_as=jnp.bfloat16):
    gain = block_scale(rng, shape, shards, -0.22, 0.18) if shards else 1.0
    entries = jax.random.normal(rng, shape, jnp.float32) * scale * gain
    return jnp.minimum(jnp.maximum(entries, -most), most).astype(held_as)


def setup_inputs(seed: int = 0, part: int = 0) -> dict:
    seeds = jax.random.split(jax.random.key(seed), 4)
    part_keys = jax.random.split(jax.random.fold_in(seeds[3], part), 4)
    coeffs = centred(part_keys[0], (PAIRS, COLS, KP), 1.0, 6.0, ((0, 64),))
    legendre = centred(seeds[1], (PAIRS, HLAT, KP), (KP // 2) ** -0.5, 0.1875, ((0, 64),))
    assign = jax.random.permutation(seeds[2], PAIRS).astype(jnp.int32)
    return {"coeffs": coeffs, "legendre": legendre, "assign": assign}


def slot_values(legendre_rows, coeff_rows, pair):
    entry = jnp.arange(KP, dtype=jnp.int32)
    first_len = (TRUNC + 1 - pair).astype(jnp.int32)
    second = entry >= first_len
    degree_gap = jnp.where(second, entry - first_len, entry)
    odd_gap = (degree_gap % 2) == 1
    group_masks = jnp.stack([
        jnp.logical_and(jnp.logical_not(second), jnp.logical_not(odd_gap)),
        jnp.logical_and(jnp.logical_not(second), odd_gap),
        jnp.logical_and(second, jnp.logical_not(odd_gap)),
        jnp.logical_and(second, odd_gap)], axis=0).astype(jnp.float32)
    masked = coeff_rows.astype(jnp.float32)[None, :, :] * group_masks[:, None, :]
    partial_value = jnp.einsum('hk,gck->hcg', legendre_rows.astype(jnp.float32), masked)
    north_rows = partial_value[:, :, 0::2] + partial_value[:, :, 1::2]
    south_rows = partial_value[:, :, 0::2] - partial_value[:, :, 1::2]
    return jnp.concatenate([north_rows, south_rows[::-1]], axis=0)


def reference(coeffs, legendre, assign):
    def one_slot(items):
        return slot_values(items[0], items[1], items[2])

    values = lax.map(one_slot, (legendre, coeffs, assign))
    values = jnp.transpose(values, (1, 2, 0, 3)).reshape(2 * HLAT, 2 * FIELDS, 2 * PAIRS)
    column = jnp.arange(2 * PAIRS, dtype=jnp.int32)
    owner_pair = assign[column // 2]
    column_place = jnp.where(column % 2 == 0, owner_pair, 2 * PAIRS - 1 - owner_pair).astype(jnp.int32)
    fourier = jnp.zeros((2 * HLAT, 2 * FIELDS, 2 * PAIRS), jnp.float32)
    return fourier.at[:, :, column_place].set(values)
```

```python
import jax
import jax.numpy as jnp
from jax import lax
from jax.experimental import pallas as pl
from jax.experimental.pallas import tpu as pltpu
from jax.sharding import PartitionSpec as P

TRUNC = 2047
MESH = pl.DeviceIdType.MESH
N = 64
SLOTS = 8
HLAT = 256
COLS = 64
KMAIN = 2048
CHUNK = 256
F32 = jnp.float32
BF16 = jnp.bfloat16
I32 = jnp.int32


def other(me, t):
    out = 0
    for b in range(6):
        bit = lax.rem(lax.div(me, 1 << b) + lax.div(t, 1 << b), 2)
        out = out + bit * (1 << b)
    return out


def place_of(d):
    south = lax.div(d, 32)
    return d + south * (95 - 2 * d)


def kernel(
    assign_hbm, coeffs_hbm, legendre_hbm, out_ref,
    pair_smem, coeffs_v, raw_v, leg_v, signed_v, send, recv, my_row, rows, vals, hot,
    pair_sem, coeffs_sem, leg_sem, send_sem, recv_sem, row_send_sem, row_recv_sem,
):
    me = lax.axis_index("ma")
    z = lax.div(me, 8)
    zhalf = lax.div(z, 4)

    pair_copy = pltpu.make_async_copy(assign_hbm, pair_smem, pair_sem)
    pair_copy.start()
    coeffs_copy = pltpu.make_async_copy(coeffs_hbm, coeffs_v, coeffs_sem)
    coeffs_copy.start()

    def leg_copy(i):
        rows_of = pl.ds(i * CHUNK, CHUNK)
        return pltpu.make_async_copy(legendre_hbm.at[rows_of], raw_v.at[rows_of], leg_sem.at[i])

    chunks = KMAIN // CHUNK
    for i in range(chunks):
        leg_copy(i).start()
    tail_copy = pltpu.make_async_copy(
        legendre_hbm.at[pl.ds(KMAIN, 1)], raw_v.at[pl.ds(KMAIN, 1)], leg_sem.at[chunks]
    )
    tail_copy.start()

    barrier = pltpu.get_barrier_semaphore()

    def greet(t, carry):
        a = lax.div(t, 8)
        plane = a * zhalf + (7 - a) * (1 - zhalf)
        d = plane * 8 + lax.rem(t, 8)
        pl.semaphore_signal(barrier, inc=1, device_id={"ma": d}, device_id_type=MESH)
        return carry

    lax.fori_loop(0, N, greet, 0)

    pair_copy.wait()
    lane = lax.broadcasted_iota(I32, (1, 128), 1)
    first_lane = lax.rem(me, 16) * SLOTS
    row = jnp.zeros((1, 128), I32)
    for s in range(SLOTS):
        row = jnp.where(lane == first_lane + s, pair_smem[s], row)
    my_row[0] = row
    rows[me] = row

    def regroup(i, carry):
        leg_copy(i).wait()
        for j in range(CHUNK // 32):
            start = pl.multiple_of(i * CHUNK + j * 32, 32)
            leg_v[:, pl.ds(start, 32), :] = jnp.transpose(raw_v[pl.ds(start, 32)], (1, 0, 2))
        return carry

    lax.fori_loop(0, chunks, regroup, 0)
    tail_copy.wait()
    coeffs_copy.wait()
    last_row = raw_v[KMAIN].astype(F32)
    slot_of = lax.broadcasted_iota(I32, (SLOTS, HLAT), 0)
    entry = lax.broadcasted_iota(I32, (1, KMAIN), 1)

    def one_slot(s, carry):
        pair = pair_smem[s]
        first_len = TRUNC + 1 - pair
        second = entry >= first_len
        sign_first = 1 - 2 * (entry & 1)
        sign_second = 1 - 2 * ((entry - first_len) & 1)
        c = coeffs_v[s, :, 0:KMAIN]
        masks = (
            jnp.where(second, 0, 1),
            jnp.where(second, 1, 0),
            jnp.where(second, 0, sign_first),
            jnp.where(second, sign_second, 0),
        )
        for g, mask in enumerate(masks):
            signed_v[g * COLS:(g + 1) * COLS, :] = c * mask.astype(F32).astype(BF16)
        part = jnp.dot(signed_v[...], leg_v[s], preferred_element_type=F32)
        leg_row = jnp.sum(jnp.where(slot_of == s, last_row, 0.0), axis=0, keepdims=True)
        edge = coeffs_v[s, :, KMAIN:KMAIN + 1].astype(F32) * leg_row
        edge_sign = (1 - 2 * (pair & 1)).astype(F32)
        north = jnp.concatenate([part[0:COLS], part[COLS:2 * COLS] + edge], axis=0)
        south = jnp.concatenate(
            [part[2 * COLS:3 * COLS], part[3 * COLS:4 * COLS] + edge * edge_sign], axis=0
        )
        mine = pl.ds(pl.multiple_of(s * 8, 8), 8)
        send[0:32, mine, :] = north.T.reshape(32, 8, 128)
        send[32:64, mine, :] = south.T.reshape(32, 8, 128)
        return carry

    lax.fori_loop(0, SLOTS, one_slot, 0)

    def block_copy(t):
        d = other(me, t)
        return pltpu.make_async_remote_copy(
            src_ref=send.at[place_of(d)], dst_ref=recv.at[me], send_sem=send_sem.at[t], recv_sem=recv_sem.at[me],
            device_id={"ma": d}, device_id_type=MESH,
        )

    def row_copy(t):
        return pltpu.make_async_remote_copy(
            src_ref=my_row.at[0], dst_ref=rows.at[me], send_sem=row_send_sem.at[t], recv_sem=row_recv_sem.at[me],
            device_id={"ma": other(me, t)}, device_id_type=MESH,
        )

    pl.semaphore_wait(barrier, N)

    def send_row(t, carry):
        row_copy(t).start()
        return carry

    def send_block(t, carry):
        block_copy(t).start()
        return carry

    lax.fori_loop(1, N, send_row, 0)
    lax.fori_loop(1, N, send_block, 0)
    recv[me] = send[place_of(me)]

    out_ref[...] = jnp.zeros_like(out_ref)
    half = lax.div(me, 32)
    column = lax.broadcasted_iota(I32, (512, 128), 0)

    def one_group(step, carry):
        late = lax.div(step, 2)
        second = lax.rem(step, 2)
        group = (1 - late) * (2 * zhalf + second) + late * (3 * (1 - zhalf) * (1 - second) + (2 - zhalf) * second)

        def arrived(i, c):
            src = group * 16 + i

            @pl.when(src != me)
            def _():
                pltpu.make_async_copy(rows.at[src], rows.at[src], row_recv_sem.at[src]).wait()
                pltpu.make_async_copy(recv.at[src], recv.at[src], recv_sem.at[src]).wait()

            return c

        lax.fori_loop(0, 16, arrived, 0)
        pairs = jnp.sum(rows[pl.ds(group * 16, 16)], axis=0)
        first_hot = jnp.where(column == pairs, 1.0, 0.0).astype(BF16)
        second_hot = jnp.where(column == 511 - pairs, 1.0, 0.0).astype(BF16)
        hot[0, :, 0:128] = first_hot
        hot[0, :, 128:256] = first_hot
        hot[1, :, 0:128] = second_hot
        hot[1, :, 128:256] = second_hot
        for i in range(8):
            r = i + half * (7 - 2 * i)
            got = jnp.concatenate(
                [recv[group * 16 + j, pl.ds(r, 8, stride=8), :] for j in range(16)], axis=0
            ).T
            high = got.astype(BF16)
            low = (got - high.astype(F32)).astype(BF16)
            for w in range(2):
                vals[w, i * COLS:(i + 1) * COLS, 0:128] = high[w * COLS:(w + 1) * COLS]
                vals[w, i * COLS:(i + 1) * COLS, 128:256] = low[w * COLS:(w + 1) * COLS]
        for w in range(2):
            out_ref[:, w * 512:(w + 1) * 512] += lax.dot_general(
                vals[w], hot[w], (((1,), (1,)), ((), ())), preferred_element_type=F32
            )
        return carry

    lax.fori_loop(0, 4, one_group, 0)

    def sent(t, carry):
        row_copy(t).wait_send()
        block_copy(t).wait_send()
        return carry

    lax.fori_loop(1, N, sent, 0)


def shards(coeffs, legendre, assign):
    leg = jnp.transpose(legendre, (2, 0, 1))
    dma = pltpu.SemaphoreType.DMA
    out = pl.pallas_call(
        kernel,
        name="synthesis",
        out_shape=jax.ShapeDtypeStruct((512, 1024), F32),
        in_specs=[pl.BlockSpec(memory_space=pltpu.HBM)] * 3,
        out_specs=pl.BlockSpec(memory_space=pltpu.VMEM),
        scratch_shapes=[
            pltpu.SMEM((SLOTS,), I32),
            pltpu.VMEM((SLOTS, COLS, KMAIN + 1), BF16),
            pltpu.VMEM((KMAIN + 1, SLOTS, HLAT), BF16),
            pltpu.VMEM((SLOTS, KMAIN, HLAT), BF16),
            pltpu.VMEM((4 * COLS, KMAIN), BF16),
            pltpu.VMEM((N, 64, 128), F32),
            pltpu.VMEM((N, 64, 128), F32),
            pltpu.VMEM((1, 1, 128), I32),
            pltpu.VMEM((N, 1, 128), I32),
            pltpu.VMEM((2, 512, 256), BF16),
            pltpu.VMEM((2, 512, 256), BF16),
            dma,
            dma,
            dma((KMAIN // CHUNK + 1,)),
            dma((N,)),
            dma((N,)),
            dma((N,)),
            dma((N,)),
        ],
        compiler_params=pltpu.CompilerParams(
            collective_id=0, has_side_effects=True, vmem_limit_bytes=44 * 2**20
        ),
    )(assign, coeffs, leg)
    return out.reshape(8, COLS, 1024)


def solution(mesh):
    return jax.shard_map(
        shards,
        mesh=mesh,
        in_specs=(P("ma", "af", None), P("ma", None, None), P("ma")),
        out_specs=P("ma", "af", None),
        check_vma=False,
    )
```

```python
import jax
import jax.numpy as jnp
from jax import lax
from jax.experimental import pallas as pl
from jax.experimental.pallas import tpu as pltpu
from jax.sharding import PartitionSpec as P

TRUNC = 2047
MESH = pl.DeviceIdType.MESH
N = 64
SLOTS = 8
HLAT = 256
COLS = 64
KMAIN = 2048
CUTS = (0, 1024, 2048)
CHUNKS = len(CUTS) - 1
CHUNK = max(b - a for a, b in zip(CUTS, CUTS[1:]))
F32 = jnp.float32
BF16 = jnp.bfloat16
I32 = jnp.int32


def other(me, t, bits):
    out = 0
    for b in range(bits):
        bit = lax.rem(lax.div(me, 1 << b) + lax.div(t, 1 << b), 2)
        out = out + bit * (1 << b)
    return out


def place_of(d):
    south = lax.div(d, 32)
    return d + south * (95 - 2 * d)


def kernel(
    assign_hbm, coeffs_hbm, legendre_hbm, out_ref,
    pair_smem, coeffs_v, raw_v, leg_v, signed_v, acc, send, recv, my_row, rows, plane_row, plane_rows, vals, hot,
    ready, pair_sem, coeffs_sem, leg_sem, send_sem, recv_sem,
    row_send_sem, row_recv_sem, plane_send_sem, plane_recv_sem,
):
    me = lax.axis_index("ma")
    z = lax.div(me, 8)
    here = lax.rem(me, 8)
    zhalf = lax.div(z, 4)

    pair_copy = pltpu.make_async_copy(assign_hbm, pair_smem, pair_sem)
    pair_copy.start()
    coeffs_copy = pltpu.make_async_copy(coeffs_hbm, coeffs_v, coeffs_sem)
    coeffs_copy.start()

    def leg_copy(i):
        rows_of = pl.ds(CUTS[i], CUTS[i + 1] - CUTS[i] + i // (CHUNKS - 1))
        return pltpu.make_async_copy(legendre_hbm.at[rows_of], raw_v.at[rows_of], leg_sem.at[i])

    for i in range(CHUNKS):
        leg_copy(i).start()

    barrier = pltpu.get_barrier_semaphore()
    for plane in reversed(range(8)):
        @pl.when(plane >= z)
        def _():
            for b in range(8):
                pl.semaphore_signal(barrier, inc=1, device_id={"ma": plane * 8 + b}, device_id_type=MESH)

    pair_copy.wait()
    lane = lax.broadcasted_iota(I32, (1, 128), 1)
    first_lane = lax.rem(me, 16) * SLOTS
    row = jnp.zeros((1, 128), I32)
    for s in range(SLOTS):
        row = jnp.where(lane == first_lane + s, pair_smem[s], row)
    my_row[0] = row
    rows[here] = row

    pl.semaphore_wait(barrier, 8 * (z + 1))
    for plane in range(7):
        @pl.when(plane < z)
        def _():
            for b in range(8):
                pl.semaphore_signal(ready.at[z], inc=1, device_id={"ma": plane * 8 + b}, device_id_type=MESH)

    def row_copy(b):
        return pltpu.make_async_remote_copy(
            src_ref=my_row.at[0], dst_ref=rows.at[here], send_sem=row_send_sem.at[b], recv_sem=row_recv_sem.at[here],
            device_id={"ma": z * 8 + b}, device_id_type=MESH,
        )

    def plane_copy(plane):
        return pltpu.make_async_remote_copy(
            src_ref=plane_row.at[0], dst_ref=plane_rows.at[z], send_sem=plane_send_sem.at[plane],
            recv_sem=plane_recv_sem.at[z], device_id={"ma": plane * 8 + here}, device_id_type=MESH,
        )

    def mates(body):
        for b in range(8):
            @pl.when(b != here)
            def _():
                body(b)

    def planes(body):
        for plane in range(8):
            @pl.when(plane != z)
            def _():
                body(plane)

    mates(lambda b: row_copy(b).start())

    coeffs_copy.wait()
    entry = lax.broadcasted_iota(I32, (1, KMAIN), 1)

    def sign(s, carry):
        first_len = TRUNC + 1 - pair_smem[s]
        second = entry >= first_len
        sign_first = 1 - 2 * (entry & 1)
        sign_second = 1 - 2 * ((entry - first_len) & 1)
        c = coeffs_v[s, :, 0:KMAIN]
        masks = (
            jnp.where(second, 0, 1),
            jnp.where(second, 1, 0),
            jnp.where(second, 0, sign_first),
            jnp.where(second, sign_second, 0),
        )
        for g, mask in enumerate(masks):
            signed_v[s, g * COLS:(g + 1) * COLS, :] = c * mask.astype(F32).astype(BF16)
        return carry

    lax.fori_loop(0, SLOTS, sign, 0)

    slot_of = lax.broadcasted_iota(I32, (SLOTS, HLAT), 0)

    def synthesize():
        for i in range(CHUNKS):
            leg_copy(i).wait()
            size = CUTS[i + 1] - CUTS[i]
            for j in range(0, size, 32):
                leg_v[:, j:j + 32, :] = jnp.transpose(raw_v[CUTS[i] + j:CUTS[i] + j + 32], (1, 0, 2))

            def add(s, carry, i=i, size=size):
                here = jnp.dot(
                    signed_v[s, :, CUTS[i]:CUTS[i + 1]], leg_v[s, 0:size], preferred_element_type=F32
                )
                if i == 0:
                    acc[s] = here
                else:
                    acc[s] += here
                return carry

            if i < CHUNKS - 1:
                lax.fori_loop(0, SLOTS, add, 0, unroll=True)

        def finish(s, carry):
            i = CHUNKS - 1
            size = CUTS[i + 1] - CUTS[i]
            total = acc[s] + jnp.dot(
                signed_v[s, :, CUTS[i]:CUTS[i + 1]], leg_v[s, 0:size], preferred_element_type=F32
            )
            last = raw_v[KMAIN].astype(F32)
            last = jnp.sum(jnp.where(slot_of == s, last, 0.0), axis=0, keepdims=True)
            edge = coeffs_v[s, :, KMAIN:KMAIN + 1].astype(F32) * last
            edge_sign = (1 - 2 * (pair_smem[s] & 1)).astype(F32)
            north = jnp.concatenate([total[0:COLS], total[COLS:2 * COLS] + edge], axis=0)
            south = jnp.concatenate(
                [total[2 * COLS:3 * COLS], total[3 * COLS:4 * COLS] + edge * edge_sign], axis=0
            )
            mine = pl.ds(pl.multiple_of(s * 8, 8), 8)
            send[0:32, mine, :] = north.T.reshape(32, 8, 128)
            send[32:64, mine, :] = south.T.reshape(32, 8, 128)
            return carry

        lax.fori_loop(0, SLOTS, finish, 0, unroll=True)

    def block_copy(d):
        return pltpu.make_async_remote_copy(
            src_ref=send.at[place_of(d)], dst_ref=recv.at[me], send_sem=send_sem.at[d], recv_sem=recv_sem.at[me],
            device_id={"ma": d}, device_id_type=MESH,
        )

    synthesize()

    mates(lambda b: pltpu.make_async_copy(rows.at[b], rows.at[b], row_recv_sem.at[b]).wait())
    pairs_here = jnp.sum(rows[...], axis=0)
    plane_row[0] = pairs_here
    plane_rows[z] = pairs_here


    for plane in range(1, 8):
        @pl.when(plane > z)
        def _():
            pl.semaphore_wait(ready.at[plane], 8)

    planes(lambda plane: plane_copy(plane).start())

    def send_rest(t, carry):
        d = other(me, lax.div(t, 2) + 32 * (1 - lax.rem(t, 2)), 6)

        @pl.when(d != me)
        def _():
            block_copy(d).start()

        return carry

    lax.fori_loop(0, N, send_rest, 0)
    recv[me] = send[place_of(me)]
    planes(lambda plane: pltpu.make_async_copy(plane_rows.at[plane], plane_rows.at[plane], plane_recv_sem.at[plane]).wait())

    out_ref[...] = jnp.zeros_like(out_ref)
    half = lax.div(me, 32)
    column = lax.broadcasted_iota(I32, (512, 128), 0)

    def one_group(step, carry):
        late = lax.div(step, 2)
        second = lax.rem(step, 2)
        group = (1 - late) * (2 * zhalf + second) + late * (3 * (1 - zhalf) * (1 - second) + (2 - zhalf) * second)

        def arrived(i, c):
            src = group * 16 + i
            @pl.when(src != me)
            def _():
                pltpu.make_async_copy(recv.at[src], recv.at[src], recv_sem.at[src]).wait()

            return c

        lax.fori_loop(0, 16, arrived, 0)
        pairs = plane_rows[2 * group] + plane_rows[2 * group + 1]
        first_hot = jnp.where(column == pairs, 1.0, 0.0).astype(BF16)
        second_hot = jnp.where(column == 511 - pairs, 1.0, 0.0).astype(BF16)
        hot[0, :, 0:128] = first_hot
        hot[0, :, 128:256] = first_hot
        hot[1, :, 0:128] = second_hot
        hot[1, :, 128:256] = second_hot
        for i in range(8):
            r = i + half * (7 - 2 * i)
            got = jnp.concatenate(
                [recv[group * 16 + j, pl.ds(r, 8, stride=8), :] for j in range(16)], axis=0
            ).T
            high = got.astype(BF16)
            low = (got - high.astype(F32)).astype(BF16)
            for w in range(2):
                vals[w, i * COLS:(i + 1) * COLS, 0:128] = high[w * COLS:(w + 1) * COLS]
                vals[w, i * COLS:(i + 1) * COLS, 128:256] = low[w * COLS:(w + 1) * COLS]
        for w in range(2):
            out_ref[:, w * 512:(w + 1) * 512] += lax.dot_general(
                vals[w], hot[w], (((1,), (1,)), ((), ())), preferred_element_type=F32
            )
        return carry

    lax.fori_loop(0, 4, one_group, 0)

    mates(lambda b: row_copy(b).wait_send())
    planes(lambda plane: plane_copy(plane).wait_send())

    def sent(d, carry):
        @pl.when(d != me)
        def _():
            block_copy(d).wait_send()

        return carry

    lax.fori_loop(0, N, sent, 0)


def shards(coeffs, legendre, assign):
    leg = jnp.transpose(legendre, (2, 0, 1))
    dma = pltpu.SemaphoreType.DMA
    out = pl.pallas_call(
        kernel,
        name="synthesis",
        out_shape=jax.ShapeDtypeStruct((512, 1024), F32),
        in_specs=[pl.BlockSpec(memory_space=pltpu.HBM)] * 3,
        out_specs=pl.BlockSpec(memory_space=pltpu.VMEM),
        scratch_shapes=[
            pltpu.SMEM((SLOTS,), I32),
            pltpu.VMEM((SLOTS, COLS, KMAIN + 1), BF16),
            pltpu.VMEM((KMAIN + 1, SLOTS, HLAT), BF16),
            pltpu.VMEM((SLOTS, CHUNK, HLAT), BF16),
            pltpu.VMEM((SLOTS, 4 * COLS, KMAIN), BF16),
            pltpu.VMEM((SLOTS, 4 * COLS, HLAT), F32),
            pltpu.VMEM((N, 64, 128), F32),
            pltpu.VMEM((N, 64, 128), F32),
            pltpu.VMEM((1, 1, 128), I32),
            pltpu.VMEM((8, 1, 128), I32),
            pltpu.VMEM((1, 1, 128), I32),
            pltpu.VMEM((8, 1, 128), I32),
            pltpu.VMEM((2, 512, 256), BF16),
            pltpu.VMEM((2, 512, 256), BF16),
            pltpu.SemaphoreType.REGULAR((8,)),
            dma,
            dma,
            dma((CHUNKS,)),
            dma((N,)),
            dma((N,)),
            dma((8,)),
            dma((8,)),
            dma((8,)),
            dma((8,)),
        ],
        compiler_params=pltpu.CompilerParams(
            collective_id=0, has_side_effects=True, vmem_limit_bytes=44 * 2**20
        ),
    )(*(pltpu.with_memory_space_constraint(x, pltpu.HBM) for x in (assign, coeffs, leg)))
    return out.reshape(8, COLS, 1024)


def solution(mesh):
    return jax.shard_map(
        shards,
        mesh=mesh,
        in_specs=(P("ma", "af", None), P("ma", None, None), P("ma")),
        out_specs=P("ma", "af", None),
        check_vma=False,
    )
```

```python
import jax
import jax.numpy as jnp
from jax import lax
from jax.experimental import pallas as pl
from jax.experimental.pallas import tpu as pltpu
from jax.sharding import PartitionSpec as P

TRUNC = 2047
MESH = pl.DeviceIdType.MESH
N = 64
SLOTS = 8
HLAT = 256
COLS = 64
KMAIN = 2048
CUTS = (0, 1280, 2048)
CHUNKS = len(CUTS) - 1
CHUNK = max(b - a for a, b in zip(CUTS, CUTS[1:]))
F32 = jnp.float32
BF16 = jnp.bfloat16
I32 = jnp.int32


def other(me, t, bits):
    out = 0
    for b in range(bits):
        bit = lax.rem(lax.div(me, 1 << b) + lax.div(t, 1 << b), 2)
        out = out + bit * (1 << b)
    return out


def place_of(d):
    south = lax.div(d, 32)
    return d + south * (95 - 2 * d)


def kernel(
    assign_hbm, coeffs_hbm, legendre_hbm, out_ref,
    pair_smem, coeffs_v, raw_v, leg_v, signed_v, acc, send, recv, my_row, rows, plane_row, plane_rows, vals, hot,
    ready, pair_sem, coeffs_sem, leg_sem, send_sem, recv_sem,
    row_send_sem, row_recv_sem, plane_send_sem, plane_recv_sem,
):
    me = lax.axis_index("ma")
    z = lax.div(me, 8)
    here = lax.rem(me, 8)
    zhalf = lax.div(z, 4)

    pair_copy = pltpu.make_async_copy(assign_hbm, pair_smem, pair_sem)
    pair_copy.start()
    coeffs_copy = pltpu.make_async_copy(coeffs_hbm, coeffs_v, coeffs_sem)
    coeffs_copy.start()

    def leg_copy(i):
        rows_of = pl.ds(CUTS[i], CUTS[i + 1] - CUTS[i] + i // (CHUNKS - 1))
        return pltpu.make_async_copy(legendre_hbm.at[rows_of], raw_v.at[rows_of], leg_sem.at[i])

    for i in range(CHUNKS):
        leg_copy(i).start()

    barrier = pltpu.get_barrier_semaphore()
    for plane in reversed(range(8)):
        @pl.when(plane >= z)
        def _():
            for b in range(8):
                pl.semaphore_signal(barrier, inc=1, device_id={"ma": plane * 8 + b}, device_id_type=MESH)

    pair_copy.wait()
    lane = lax.broadcasted_iota(I32, (1, 128), 1)
    first_lane = lax.rem(me, 16) * SLOTS
    row = jnp.zeros((1, 128), I32)
    for s in range(SLOTS):
        row = jnp.where(lane == first_lane + s, pair_smem[s], row)
    my_row[0] = row
    rows[here] = row

    pl.semaphore_wait(barrier, 8 * (z + 1))
    for plane in range(7):
        @pl.when(plane < z)
        def _():
            for b in range(8):
                pl.semaphore_signal(ready.at[z], inc=1, device_id={"ma": plane * 8 + b}, device_id_type=MESH)

    def row_copy(b):
        return pltpu.make_async_remote_copy(
            src_ref=my_row.at[0], dst_ref=rows.at[here], send_sem=row_send_sem.at[b], recv_sem=row_recv_sem.at[here],
            device_id={"ma": z * 8 + b}, device_id_type=MESH,
        )

    def plane_copy(plane):
        return pltpu.make_async_remote_copy(
            src_ref=plane_row.at[0], dst_ref=plane_rows.at[z], send_sem=plane_send_sem.at[plane],
            recv_sem=plane_recv_sem.at[z], device_id={"ma": plane * 8 + here}, device_id_type=MESH,
        )

    def mates(body):
        for b in range(8):
            @pl.when(b != here)
            def _():
                body(b)

    def planes(body):
        for plane in range(8):
            @pl.when(plane != z)
            def _():
                body(plane)

    mates(lambda b: row_copy(b).start())

    coeffs_copy.wait()
    entry = lax.broadcasted_iota(I32, (1, KMAIN), 1)

    def sign(s, carry):
        first_len = TRUNC + 1 - pair_smem[s]
        second = entry >= first_len
        sign_first = 1 - 2 * (entry & 1)
        sign_second = 1 - 2 * ((entry - first_len) & 1)
        c = coeffs_v[s, :, 0:KMAIN]
        masks = (
            jnp.where(second, 0, 1),
            jnp.where(second, 1, 0),
            jnp.where(second, 0, sign_first),
            jnp.where(second, sign_second, 0),
        )
        for g, mask in enumerate(masks):
            signed_v[s, g * COLS:(g + 1) * COLS, :] = c * mask.astype(F32).astype(BF16)
        return carry

    lax.fori_loop(0, SLOTS, sign, 0)

    slot_of = lax.broadcasted_iota(I32, (SLOTS, HLAT), 0)

    def synthesize():
        for i in range(CHUNKS):
            leg_copy(i).wait()
            size = CUTS[i + 1] - CUTS[i]
            for j in range(0, size, 32):
                leg_v[:, j:j + 32, :] = jnp.transpose(raw_v[CUTS[i] + j:CUTS[i] + j + 32], (1, 0, 2))

            def add(s, carry, i=i, size=size):
                here = jnp.dot(
                    signed_v[s, :, CUTS[i]:CUTS[i + 1]], leg_v[s, 0:size], preferred_element_type=F32
                )
                if i == 0:
                    acc[s] = here
                else:
                    acc[s] += here
                return carry

            if i < CHUNKS - 1:
                lax.fori_loop(0, SLOTS, add, 0, unroll=True)

        def finish(s, carry):
            i = CHUNKS - 1
            size = CUTS[i + 1] - CUTS[i]
            total = acc[s] + jnp.dot(
                signed_v[s, :, CUTS[i]:CUTS[i + 1]], leg_v[s, 0:size], preferred_element_type=F32
            )
            last = raw_v[KMAIN].astype(F32)
            last = jnp.sum(jnp.where(slot_of == s, last, 0.0), axis=0, keepdims=True)
            edge = coeffs_v[s, :, KMAIN:KMAIN + 1].astype(F32) * last
            edge_sign = (1 - 2 * (pair_smem[s] & 1)).astype(F32)
            north = jnp.concatenate([total[0:COLS], total[COLS:2 * COLS] + edge], axis=0)
            south = jnp.concatenate(
                [total[2 * COLS:3 * COLS], total[3 * COLS:4 * COLS] + edge * edge_sign], axis=0
            )
            mine = pl.ds(pl.multiple_of(s * 8, 8), 8)
            send[0:32, mine, :] = north.T.reshape(32, 8, 128)
            send[32:64, mine, :] = south.T.reshape(32, 8, 128)
            return carry

        lax.fori_loop(0, SLOTS, finish, 0, unroll=True)

    def block_copy(d):
        return pltpu.make_async_remote_copy(
            src_ref=send.at[place_of(d)], dst_ref=recv.at[me], send_sem=send_sem.at[d], recv_sem=recv_sem.at[me],
            device_id={"ma": d}, device_id_type=MESH,
        )

    synthesize()

    mates(lambda b: pltpu.make_async_copy(rows.at[b], rows.at[b], row_recv_sem.at[b]).wait())
    pairs_here = jnp.sum(rows[...], axis=0)
    plane_row[0] = pairs_here
    plane_rows[z] = pairs_here


    for plane in range(1, 8):
        @pl.when(jnp.logical_and(plane > z, zhalf == plane // 4))
        def _():
            pl.semaphore_wait(ready.at[plane], 8)


    for plane in range(8):
        @pl.when(jnp.logical_and(plane != z, plane < 4 * (zhalf + 1)))
        def _():
            plane_copy(plane).start()

    def send_pair(t, carry):
        e = lax.div(t, 8)
        plane = other(z, 4 + e + (1 - zhalf) * (4 * (1 - lax.min(e, 1)) - 1), 3)

        @pl.when(jnp.logical_and(lax.rem(t, 8) == 0, zhalf == 0))
        def _():
            pl.semaphore_wait(ready.at[plane], 8)
            plane_copy(plane).start()

        block_copy(plane * 8 + other(here, lax.rem(t, 8), 3)).start()
        d = other(me, t, 5) + 32 * zhalf

        @pl.when(d != me)
        def _():
            block_copy(d).start()

        return carry

    lax.fori_loop(0, N // 2, send_pair, 0)
    recv[me] = send[place_of(me)]
    planes(lambda plane: pltpu.make_async_copy(plane_rows.at[plane], plane_rows.at[plane], plane_recv_sem.at[plane]).wait())

    out_ref[...] = jnp.zeros_like(out_ref)
    half = lax.div(me, 32)
    column = lax.broadcasted_iota(I32, (512, 128), 0)

    def sent(d, carry):
        @pl.when(d != me)
        def _():
            block_copy(d).wait_send()

        return carry

    def one_group(step, carry):
        late = lax.div(step, 2)
        second = lax.rem(step, 2)
        group = (1 - late) * (2 * zhalf + second) + late * (3 * (1 - zhalf) * (1 - second) + (2 - zhalf) * second)

        def arrived(i, c):
            src = group * 16 + i
            @pl.when(src != me)
            def _():
                pltpu.make_async_copy(recv.at[src], recv.at[src], recv_sem.at[src]).wait()

            return c

        pairs = plane_rows[2 * group] + plane_rows[2 * group + 1]
        first_hot = jnp.where(column == pairs, 1.0, 0.0).astype(BF16)
        second_hot = jnp.where(column == 511 - pairs, 1.0, 0.0).astype(BF16)
        hot[0, :, 0:128] = first_hot
        hot[0, :, 128:256] = first_hot
        hot[1, :, 0:128] = second_hot
        hot[1, :, 128:256] = second_hot

        @pl.when(step == 3)
        def _():
            mates(lambda b: row_copy(b).wait_send())
            planes(lambda plane: plane_copy(plane).wait_send())
            lax.fori_loop(0, N, sent, 0)

        lax.fori_loop(0, 16, arrived, 0)
        for i in range(8):
            r = i + half * (7 - 2 * i)
            got = jnp.concatenate(
                [recv[group * 16 + j, pl.ds(r, 8, stride=8), :] for j in range(16)], axis=0
            ).T
            high = got.astype(BF16)
            low = (got - high.astype(F32)).astype(BF16)
            for w in range(2):
                vals[w, i * COLS:(i + 1) * COLS, 0:128] = high[w * COLS:(w + 1) * COLS]
                vals[w, i * COLS:(i + 1) * COLS, 128:256] = low[w * COLS:(w + 1) * COLS]
        for w in range(2):
            out_ref[:, w * 512:(w + 1) * 512] += lax.dot_general(
                vals[w], hot[w], (((1,), (1,)), ((), ())), preferred_element_type=F32
            )
        return carry

    lax.fori_loop(0, 4, one_group, 0)


def shards(coeffs, legendre, assign):
    leg = jnp.transpose(legendre, (2, 0, 1))
    dma = pltpu.SemaphoreType.DMA
    out = pl.pallas_call(
        kernel,
        name="synthesis",
        out_shape=jax.ShapeDtypeStruct((512, 1024), F32),
        in_specs=[pl.BlockSpec(memory_space=pltpu.HBM)] * 3,
        out_specs=pl.BlockSpec(memory_space=pltpu.VMEM),
        scratch_shapes=[
            pltpu.SMEM((SLOTS,), I32),
            pltpu.VMEM((SLOTS, COLS, KMAIN + 1), BF16),
            pltpu.VMEM((KMAIN + 1, SLOTS, HLAT), BF16),
            pltpu.VMEM((SLOTS, CHUNK, HLAT), BF16),
            pltpu.VMEM((SLOTS, 4 * COLS, KMAIN), BF16),
            pltpu.VMEM((SLOTS, 4 * COLS, HLAT), F32),
            pltpu.VMEM((N, 64, 128), F32),
            pltpu.VMEM((N, 64, 128), F32),
            pltpu.VMEM((1, 1, 128), I32),
            pltpu.VMEM((8, 1, 128), I32),
            pltpu.VMEM((1, 1, 128), I32),
            pltpu.VMEM((8, 1, 128), I32),
            pltpu.VMEM((2, 512, 256), BF16),
            pltpu.VMEM((2, 512, 256), BF16),
            pltpu.SemaphoreType.REGULAR((8,)),
            dma,
            dma,
            dma((CHUNKS,)),
            dma((N,)),
            dma((N,)),
            dma((8,)),
            dma((8,)),
            dma((8,)),
            dma((8,)),
        ],
        compiler_params=pltpu.CompilerParams(
            collective_id=0, has_side_effects=True, vmem_limit_bytes=44 * 2**20
        ),
    )(*(pltpu.with_memory_space_constraint(x, pltpu.HBM) for x in (assign, coeffs, leg)))
    return out.reshape(8, COLS, 1024)


def solution(mesh):
    return jax.shard_map(
        shards,
        mesh=mesh,
        in_specs=(P("ma", "af", None), P("ma", None, None), P("ma")),
        out_specs=P("ma", "af", None),
        check_vma=False,
    )
```
